128 devices in a mesh: row: 8 (over z, core), col: 16 (over y, x).
Axes of the slice: x: 4, y: 4, z: 4, core: 2. Of those that a mesh axis runs over, the one named last changes fastest.
Arguments:
- kernel: bfloat16 [16384, 16384], P('row', 'col'), may hold values from -6 to 6
- labels: int32 [3, 16384], replicated, may hold values from 0 to 63, as said below
Outputs:
- distance: float32 [3, 16384, 64], P(None, ('row', 'col'))
- objective: float32 [3], replicated
The draws below stay inside these ranges and needn't reach their ends.
Inputs may be any that keep to these rules, and one draw needn't show every extreme that they name: `labels`: in every iteration every cluster of 0 to 63 is named by at least one series.
All inputs are finite; a program needn't handle non-finite values.
Results may differ from the reference program's by a relative error of at most 0.0003.
Values sent between devices are 32-bit elements; how exact they have to be, the bound alone decides.
No kernel may reach another device: no remote copies, remote signals or barrier semaphores. Data moves between devices by JAX's collectives and lax.ppermute only.
A program may use at most 64 MiB of HBM per device.

```python
import jax
import jax.numpy as jnp

SERIES = 16384
CLUSTERS = 64
ITERS = 3


def draw_labels(key, part):
    rows = []
    for step in range(ITERS):
        folded = jax.random.fold_in(key, 7919 + step)
        first, second, third, fourth = jax.random.split(folded, 4)
        drawn = jax.random.randint(first, (SERIES,), 0, CLUSTERS)
        other = jax.random.randint(second, (SERIES,), 0, CLUSTERS)
        pick = jax.random.randint(third, (SERIES,), 0, 2)
        chosen = jnp.where(pick == 1, jnp.minimum(drawn, other), drawn)
        places = jax.random.permutation(fourth, SERIES)[:CLUSTERS]
        chosen = chosen.at[places].set(jnp.arange(CLUSTERS, dtype=jnp.int32))
        rows.append(chosen.astype(jnp.int32))
    return jnp.stack(rows)


def with_spikes(array, key, source, target, blocks, factor):
    owner, partner = [(jnp.arange(array.shape[position]) // (array.shape[position] // blocks)).reshape([-1 if axis == position else 1 for axis in range(array.ndim)]) for position in (source, target)]
    chosen = jax.random.permutation(key, blocks)[partner]
    strong = (owner == chosen) | (owner == (partner + blocks // 2) % blocks)
    return jnp.where(strong, factor * array, array)


def level_of(rng, extent, cuts, smallest, largest):
    gain, own = 1.0, jax.random.fold_in(rng, 6)
    for axis_at, shards_of in cuts:
        steps = jnp.exp(jax.random.uniform(jax.random.fold_in(own, axis_at), (shards_of,), jnp.float32, smallest / len(cuts), largest / len(cuts)))
        gain = gain * jnp.repeat(steps, extent[axis_at] // shards_of).reshape([-1 if axis == axis_at else 1 for axis in range(len(extent))])
    return gain


def bell_draw_with(own_key, shape, scale, most, pieces, heavy, held_as=jnp.bfloat16):
    array = scale * jax.random.normal(own_key, shape, jnp.float32)
    if pieces:
        array = array * level_of(own_key, shape, pieces, -0.22, 0.18)
    return jnp.clip(with_spikes(array, jax.random.fold_in(own_key, 3), *heavy), -most, most).astype(held_as)


def setup_inputs(seed: int = 0) -> dict:
    arg_keys = jax.random.split(jax.random.key(seed), 3)
    return {
        "kernel": bell_draw_with(arg_keys[0], (SERIES, SERIES), 1.0, 6.0, ((0, 8), (1, 16)), (1, 0, 16, 2.0)),
        "labels": draw_labels(jax.random.fold_in(arg_keys[2], 71), 0),
    }


def reference(kernel, labels):
    clusters = jnp.arange(CLUSTERS, dtype=jnp.int32)
    dists = []
    objs = []
    for step in range(ITERS):
        onehot = (labels[step][:, None] == clusters[None, :]).astype(jnp.bfloat16)
        sums = jnp.dot(kernel, onehot, preferred_element_type=jnp.float32)
        weights = onehot.astype(jnp.float32)
        counts = jnp.sum(weights, axis=0)
        totals = jnp.sum(weights * sums, axis=0)
        dists.append((-2.0 * sums) / counts[None, :] + totals[None, :] / (counts * counts)[None, :])
        objs.append(1.0 - jnp.sum(totals / counts) / SERIES)
    return jnp.stack(dists), jnp.stack(objs)
```

```python
import functools

import jax
import jax.numpy as jnp
from jax import lax
from jax.sharding import Mesh
from jax.sharding import PartitionSpec as P

SERIES = 16384
CLUSTERS = 64
ITERS = 3
COL = ("col_0", "col_1")
ROW = ("row_0", "row_1")
ROW_COL = ("row_0", "row_1", "col_0", "col_1")


def cut_along(array, dim, devices):
    before, after = (array.shape[:dim], array.shape[dim + 1 :])
    return jnp.moveaxis(array.reshape(*before, devices, -1, *after), dim, 0)


def summed_on_arrival(array, axis, dim):
    devices = lax.axis_size(axis)
    blocks = lax.all_to_all(cut_along(array, dim, devices), axis, 0, 0, tiled=True)
    return jnp.sum(blocks, axis=0)


def over_axes(array, axes):
    return functools.reduce(lax.psum, axes, array)


def shards(kernel, labels):
    rows_block, cols_block = kernel.shape
    slice_rows = rows_block // lax.axis_size(COL)
    row_base = lax.axis_index(ROW) * rows_block
    col_base = lax.axis_index(COL) * cols_block
    clusters = jnp.arange(CLUSTERS, dtype=jnp.int32)
    col_labels = lax.dynamic_slice_in_dim(labels, col_base, cols_block, 1)
    block_labels = lax.dynamic_slice_in_dim(labels, row_base, rows_block, 1)
    counts = jnp.sum((labels[:, :, None] == clusters).astype(jnp.float32), axis=1)

    def encode(chosen):
        flat = chosen.T[:, :, None] == clusters[None, None, :]
        return flat.reshape(chosen.shape[1], -1).astype(jnp.bfloat16)

    partial = jnp.dot(kernel, encode(col_labels), preferred_element_type=jnp.float32)
    weights = encode(block_labels).astype(jnp.float32)
    totals = over_axes(jnp.sum(weights * partial, axis=0), ROW_COL)
    sums = summed_on_arrival(partial, COL, 0)
    sums = sums.reshape(slice_rows, ITERS, CLUSTERS).transpose(1, 0, 2)
    totals = totals.reshape(ITERS, CLUSTERS)
    distance = -2.0 * sums / counts[:, None, :] + totals[:, None, :] / (counts * counts)[:, None, :]
    objective = 1.0 - jnp.sum(totals / counts, axis=1) / SERIES
    return (distance, objective)


def solution(mesh):
    finer = Mesh(mesh.devices.reshape(4, 2, 4, 4), ("row_0", "row_1", "col_0", "col_1"))
    return jax.shard_map(
        shards,
        mesh=finer,
        in_specs=(P(ROW, COL), P()),
        out_specs=(P(None, ROW_COL, None), P()),
        check_vma=False,
    )
```

```python
import jax
import jax.numpy as jnp
from jax import lax
from jax.experimental import pallas as pl
from jax.experimental.pallas import tpu as pltpu
from jax.sharding import Mesh
from jax.sharding import PartitionSpec as P


SERIES = 16384
CLUSTERS = 64
ITERS = 3
WIDTH = ITERS * CLUSTERS
SLICE = 128
WAVES = ((0, 4), (4, 8), (12, 4))
AXES = ("z", "k", "y", "x")


def index(z, k, y, x):
    return ((z * 2 + k) * 4 + y) * 4 + x


PLACES = [(z, k, y, x) for z in range(4) for k in range(2) for y in range(4) for x in range(4)]


def first_stage(d):
    return [(index(z, k, y, x), index(z, k, y ^ (d * k), x ^ (d * (1 - k)))) for z, k, y, x in PLACES]


def second_stage(d):
    return [(index(z, k, y, x), index(z, k, y ^ (d * (1 - k)), x ^ (d * k))) for z, k, y, x in PLACES]


def partial_sums(place, kernel, labels, *refs):
    parts, totals = refs[:4], refs[4]
    held, cols, rows, sems = refs[5:]
    depth = cols.shape[1]
    zk, at = place[0] // 16, place[0] % 16
    k, y, x = zk % 2, at // 4, at % 4
    starts = []
    for d in range(4):
        for e in range(4):
            outer, inner = y ^ jnp.where(k == 0, e, d), x ^ jnp.where(k == 0, d, e)
            starts.append(pl.multiple_of((outer * 4 + inner) * SLICE, SLICE))
    row_base = pl.multiple_of(zk * rows.shape[1], SLICE)
    col_base = pl.multiple_of(at * depth, SLICE)
    copies = [
        pltpu.make_async_copy(labels.at[:, pl.ds(col_base, cols.shape[1])], cols, sems.at[16]),
        pltpu.make_async_copy(labels.at[:, pl.ds(row_base, rows.shape[1])], rows, sems.at[17]),
    ]
    blocks = []
    for step in range(16):
        blocks.append(
            pltpu.make_async_copy(kernel.at[pl.ds(starts[step], SLICE), :], held.at[step], sems.at[step])
        )
    for copy in copies + blocks:
        copy.start()
    copies[0].wait()
    wide = lax.broadcasted_iota(jnp.int32, (CLUSTERS, depth), 0)
    onehot = jnp.concatenate(
        [(wide == cols[t : t + 1, :]).astype(jnp.float32).astype(jnp.bfloat16) for t in range(ITERS)]
    )
    copies[1].wait()
    narrow = lax.broadcasted_iota(jnp.int32, (CLUSTERS, SLICE), 0)
    sums = [jnp.zeros((CLUSTERS, SLICE), jnp.float32) for _ in range(ITERS)]
    for step, size in WAVES:
        for one in range(step, step + size):
            blocks[one].wait()
        wave = lax.dot_general(
            onehot,
            held[step : step + size].reshape(size * SLICE, depth),
            (((1,), (1,)), ((), ())),
            preferred_element_type=jnp.float32,
        )
        for one in range(step, step + size):
            part = wave[:, (one - step) * SLICE : (one - step + 1) * SLICE]
            parts[one // 4][one % 4] = part
            for t in range(ITERS):
                chosen = narrow == rows[t : t + 1, pl.ds(starts[one], SLICE)]
                sums[t] += jnp.where(chosen, part[t * CLUSTERS : (t + 1) * CLUSTERS], 0.0)
    lines = [jnp.sum(a.T, axis=0, keepdims=True) for a in sums]
    lines.append(jnp.zeros((1, CLUSTERS), jnp.float32))
    both = jnp.concatenate([jnp.concatenate(lines[0:4:2]), jnp.concatenate(lines[1:4:2])], axis=1)
    totals[...] = jnp.broadcast_to(both, totals.shape)


def stage_sum(a, b, c, d, *outs):
    for e in range(4):
        outs[e][...] = (a[e] + b[e]) + (c[e] + d[e])


def tally(labels, after, counts):
    del after
    octet = lax.broadcasted_iota(jnp.int32, (8, SERIES), 0)
    spread = lax.broadcasted_iota(jnp.int32, (8, CLUSTERS), 1) // 8
    keep = spread == lax.broadcasted_iota(jnp.int32, (8, CLUSTERS), 0)
    for t in range(ITERS):
        line = labels[t : t + 1, :]
        high = (octet == line >> 3).astype(jnp.float32).astype(jnp.bfloat16)
        low = (octet == (line & 7)).astype(jnp.float32).astype(jnp.bfloat16)
        square = lax.dot_general(
            high, low, (((1,), (1,)), ((), ())), preferred_element_type=jnp.float32
        )
        row = jnp.sum(jnp.where(keep, jnp.concatenate([square] * 8, axis=1), 0.0), axis=0, keepdims=True)
        counts[t] = jnp.broadcast_to(row, (SLICE, CLUSTERS)).T


def finish(a, b, c, d, counts, shares, distance, objective):
    sums = (a[...] + b[...]) + (c[...] + d[...])
    whole = jnp.sum(shares[...], axis=0)
    whole = (whole[0:2] + whole[2:4]) + (whole[4:6] + whole[6:8])
    for t in range(ITERS):
        row = whole[t // 2 : t // 2 + 1, t % 2 * CLUSTERS : (t % 2 + 1) * CLUSTERS]
        totals = jnp.broadcast_to(row, (SLICE, CLUSTERS)).T
        count = counts[t]
        block = sums[t * CLUSTERS : (t + 1) * CLUSTERS]
        distance[t] = (-2.0 * block) / count + totals / (count * count)
        objective[t] = 1.0 - jnp.sum((totals / count)[:, 0:1]) / SERIES


def near(array):
    return pltpu.with_memory_space_constraint(array, pltpu.VMEM)


def vmem():
    return pl.BlockSpec(memory_space=pltpu.VMEM)


def shards(kernel, labels):
    rows_block, cols_block = kernel.shape
    place = lax.axis_index(AXES).reshape(1).astype(jnp.int32)
    block = pltpu.VMEM((4, WIDTH, SLICE), jnp.float32)
    small = pltpu.VMEM((WIDTH, SLICE), jnp.float32)
    *parts, totals = pl.pallas_call(
        partial_sums,
        out_shape=[block] * 4 + [pltpu.VMEM((len(PLACES), 2, SLICE), jnp.float32)],
        in_specs=[
            pl.BlockSpec(memory_space=pltpu.SMEM),
            pl.BlockSpec(memory_space=pl.ANY),
            pl.BlockSpec(memory_space=pl.ANY),
        ],
        out_specs=[vmem()] * 5,
        scratch_shapes=[
            pltpu.VMEM((16, SLICE, cols_block), jnp.bfloat16),
            pltpu.VMEM((ITERS, cols_block), jnp.int32),
            pltpu.VMEM((ITERS, rows_block), jnp.int32),
            pltpu.SemaphoreType.DMA((18,)),
        ],
    )(place, kernel, labels)
    moved = [parts[0]] + [lax.ppermute(parts[s], AXES, first_stage(s)) for s in (1, 3, 2)]
    halves = pl.pallas_call(
        stage_sum, out_shape=[small] * 4, in_specs=[vmem()] * 4, out_specs=[vmem()] * 4
    )(*map(near, moved))
    last = [halves[0]]
    for s in (2, 1, 3):
        last.append(lax.ppermute(halves[s], AXES, second_stage(s)))
    counts = pl.pallas_call(
        tally,
        out_shape=pltpu.VMEM((ITERS, CLUSTERS, SLICE), jnp.float32),
        in_specs=[vmem()] * 2,
        out_specs=vmem(),
    )(labels, near(halves[0]))
    shares = lax.all_to_all(totals, AXES, 0, 0, tiled=True)
    shares = shares.reshape(len(PLACES) // 4, 8, SLICE)
    distance, objective = pl.pallas_call(
        finish,
        out_shape=[
            jax.ShapeDtypeStruct((ITERS, CLUSTERS, SLICE), jnp.float32),
            jax.ShapeDtypeStruct((ITERS,), jnp.float32),
        ],
        in_specs=[vmem()] * 6,
        out_specs=[vmem(), pl.BlockSpec(memory_space=pltpu.SMEM)],
    )(*map(near, last), near(counts), near(shares))
    return jnp.swapaxes(distance, 1, 2), objective


def solution(mesh):
    finer = Mesh(mesh.devices.reshape(4, 2, 4, 4), AXES)
    return jax.shard_map(
        shards,
        mesh=finer,
        in_specs=(P(("z", "k"), ("y", "x")), P()),
        out_specs=(P(None, AXES, None), P()),
        check_vma=False,
    )
```

```python
import jax
import jax.numpy as jnp
from jax import lax
from jax.experimental import pallas as pl
from jax.experimental.pallas import tpu as pltpu
from jax.sharding import Mesh
from jax.sharding import PartitionSpec as P


SERIES = 16384
CLUSTERS = 64
ITERS = 3
WIDTH = ITERS * CLUSTERS
SLICE = 128
WAVES = ((0, 4), (4, 8), (12, 4))
AXES = ("z", "k", "y", "x")


def index(z, k, y, x):
    return ((z * 2 + k) * 4 + y) * 4 + x


PLACES = [(z, k, y, x) for z in range(4) for k in range(2) for y in range(4) for x in range(4)]


def first_stage(d):
    return [(index(z, k, y, x), index(z, k, y ^ (d * k), x ^ (d * (1 - k)))) for z, k, y, x in PLACES]


def second_stage(d):
    return [(index(z, k, y, x), index(z, k, y ^ (d * (1 - k)), x ^ (d * k))) for z, k, y, x in PLACES]


def partial_sums(place, kernel, labels, *refs):
    parts, totals = refs[:4], refs[4]
    held, cols, rows, sems = refs[5:]
    depth = cols.shape[1]
    zk, at = place[0] // 16, place[0] % 16
    k, y, x = zk % 2, at // 4, at % 4
    starts = []
    for d in range(4):
        for e in range(4):
            outer, inner = y ^ jnp.where(k == 0, e, d), x ^ jnp.where(k == 0, d, e)
            starts.append(pl.multiple_of((outer * 4 + inner) * SLICE, SLICE))
    row_base = pl.multiple_of(zk * rows.shape[1], SLICE)
    col_base = pl.multiple_of(at * depth, SLICE)
    copies = [
        pltpu.make_async_copy(labels.at[:, pl.ds(col_base, cols.shape[1])], cols, sems.at[16]),
        pltpu.make_async_copy(labels.at[:, pl.ds(row_base, rows.shape[1])], rows, sems.at[17]),
    ]
    blocks = []
    for step in range(16):
        blocks.append(
            pltpu.make_async_copy(kernel.at[pl.ds(starts[step], SLICE), :], held.at[step], sems.at[step])
        )
    for copy in copies + blocks:
        copy.start()
    copies[0].wait()
    wide = lax.broadcasted_iota(jnp.int32, (CLUSTERS, depth), 0)
    onehot = jnp.concatenate(
        [(wide == cols[t : t + 1, :]).astype(jnp.float32).astype(jnp.bfloat16) for t in range(ITERS)]
    )
    copies[1].wait()
    narrow = lax.broadcasted_iota(jnp.int32, (CLUSTERS, SLICE), 0)
    sums = [jnp.zeros((CLUSTERS, SLICE), jnp.float32) for _ in range(ITERS)]
    for step, size in WAVES:
        for one in range(step, step + size):
            blocks[one].wait()
        wave = lax.dot_general(
            onehot,
            held[step : step + size].reshape(size * SLICE, depth),
            (((1,), (1,)), ((), ())),
            preferred_element_type=jnp.float32,
        )
        for one in range(step, step + size):
            part = wave[:, (one - step) * SLICE : (one - step + 1) * SLICE]
            parts[one // 4][one % 4] = part
            for t in range(ITERS):
                chosen = narrow == rows[t : t + 1, pl.ds(starts[one], SLICE)]
                sums[t] += jnp.where(chosen, part[t * CLUSTERS : (t + 1) * CLUSTERS], 0.0)
    lines = [jnp.sum(a.T, axis=0, keepdims=True) for a in sums]
    lines.append(jnp.zeros((1, CLUSTERS), jnp.float32))
    both = jnp.concatenate([jnp.concatenate(lines[0:4:2]), jnp.concatenate(lines[1:4:2])], axis=1)
    totals[...] = both


def stage_sum(a, b, c, d, *outs):
    for e in range(4):
        outs[e][...] = (a[e] + b[e]) + (c[e] + d[e])


def tally(labels, after, counts):
    del after
    octet = lax.broadcasted_iota(jnp.int32, (8, SERIES), 0)
    spread = lax.broadcasted_iota(jnp.int32, (8, CLUSTERS), 1) // 8
    keep = spread == lax.broadcasted_iota(jnp.int32, (8, CLUSTERS), 0)
    for t in range(ITERS):
        line = labels[t : t + 1, :]
        high = (octet == line >> 3).astype(jnp.float32).astype(jnp.bfloat16)
        low = (octet == (line & 7)).astype(jnp.float32).astype(jnp.bfloat16)
        square = lax.dot_general(
            high, low, (((1,), (1,)), ((), ())), preferred_element_type=jnp.float32
        )
        row = jnp.sum(jnp.where(keep, jnp.concatenate([square] * 8, axis=1), 0.0), axis=0, keepdims=True)
        counts[t] = jnp.broadcast_to(row, (SLICE, CLUSTERS)).T


def finish(a, b, c, d, counts, shares, distance, objective):
    sums = (a[...] + b[...]) + (c[...] + d[...])
    whole = jnp.sum(shares[...], axis=0)
    whole = (whole[0:2] + whole[2:4]) + (whole[4:6] + whole[6:8])
    for t in range(ITERS):
        row = whole[t // 2 : t // 2 + 1, t % 2 * CLUSTERS : (t % 2 + 1) * CLUSTERS]
        totals = jnp.broadcast_to(row, (SLICE, CLUSTERS)).T
        count = counts[t]
        block = sums[t * CLUSTERS : (t + 1) * CLUSTERS]
        distance[t] = (-2.0 * block) / count + totals / (count * count)
        objective[t] = 1.0 - jnp.sum((totals / count)[:, 0:1]) / SERIES


def near(array):
    return pltpu.with_memory_space_constraint(array, pltpu.VMEM)


def early(part, s):
    return lax.ppermute(part, AXES, first_stage(s))


def vmem():
    return pl.BlockSpec(memory_space=pltpu.VMEM)


def shards(kernel, labels):
    rows_block, cols_block = kernel.shape
    place = lax.axis_index(AXES).reshape(1).astype(jnp.int32)
    block = pltpu.VMEM((4, WIDTH, SLICE), jnp.float32)
    small = pltpu.VMEM((WIDTH, SLICE), jnp.float32)
    *parts, totals = pl.pallas_call(
        partial_sums,
        out_shape=[block] * 4 + [pltpu.VMEM((2, SLICE), jnp.float32)],
        in_specs=[
            pl.BlockSpec(memory_space=pltpu.SMEM),
            pl.BlockSpec(memory_space=pl.ANY),
            pl.BlockSpec(memory_space=pl.ANY),
        ],
        out_specs=[vmem()] * 5,
        scratch_shapes=[
            pltpu.VMEM((16, SLICE, cols_block), jnp.bfloat16),
            pltpu.VMEM((ITERS, cols_block), jnp.int32),
            pltpu.VMEM((ITERS, rows_block), jnp.int32),
            pltpu.SemaphoreType.DMA((18,)),
        ],
    )(place, kernel, labels)
    other = lax.ppermute(totals, "k", [(0, 1), (1, 0)])
    chip = totals + other
    moved = [parts[0]] + [early(parts[s], s) for s in (1, 3, 2)]
    halves = pl.pallas_call(
        stage_sum, out_shape=[small] * 4, in_specs=[vmem()] * 4, out_specs=[vmem()] * 4
    )(*map(near, moved))
    last = [halves[0]]
    for s in (2, 3, 1):
        last.append(lax.ppermute(halves[s], AXES, second_stage(s)))
    counts = pl.pallas_call(
        tally,
        out_shape=pltpu.VMEM((ITERS, CLUSTERS, SLICE), jnp.float32),
        in_specs=[vmem()] * 2,
        out_specs=vmem(),
    )(labels, near(halves[0]))
    shares = lax.all_to_all(
        jnp.broadcast_to(chip[None], (64, 2, SLICE)), ("z", "y", "x"), 0, 0, tiled=True
    )
    shares = shares.reshape(16, 8, SLICE)
    distance, objective = pl.pallas_call(
        finish,
        out_shape=[
            jax.ShapeDtypeStruct((ITERS, CLUSTERS, SLICE), jnp.float32),
            jax.ShapeDtypeStruct((ITERS,), jnp.float32),
        ],
        in_specs=[vmem()] * 6,
        out_specs=[vmem(), pl.BlockSpec(memory_space=pltpu.SMEM)],
    )(*map(near, last), near(counts), near(shares))
    return jnp.swapaxes(distance, 1, 2), objective


def solution(mesh):
    finer = Mesh(mesh.devices.reshape(4, 2, 4, 4), AXES)
    return jax.shard_map(
        shards,
        mesh=finer,
        in_specs=(P(("z", "k"), ("y", "x")), P()),
        out_specs=(P(None, AXES, None), P()),
        check_vma=False,
    )
```

```python
import jax
import jax.numpy as jnp
from jax import lax
from jax.experimental import pallas as pl
from jax.experimental.pallas import tpu as pltpu
from jax.sharding import Mesh
from jax.sharding import PartitionSpec as P


SERIES = 16384
CLUSTERS = 64
ITERS = 3
WIDTH = ITERS * CLUSTERS
SLICE = 128
WAVES = ((0, 4), (4, 8), (12, 4))
AXES = ("z", "k", "y", "x")


def index(z, k, y, x):
    return ((z * 2 + k) * 4 + y) * 4 + x


PLACES = [(z, k, y, x) for z in range(4) for k in range(2) for y in range(4) for x in range(4)]


def first_stage(d):
    return [(index(z, k, y, x), index(z, k, y ^ (d * k), x ^ (d * (1 - k)))) for z, k, y, x in PLACES]


def second_stage(d):
    return [(index(z, k, y, x), index(z, k, y ^ (d * (1 - k)), x ^ (d * k))) for z, k, y, x in PLACES]


def classes(key):
    found = {}
    for place in PLACES:
        found.setdefault(key(*place), []).append(index(*place))
    return [sorted(found[name], key=FIRST) for name in sorted(found)]


FIRST = lambda n: (n not in (index(3, 0, 2, 1), index(1, 1, 1, 2)), n)
HOPS = []
GROUPS = classes(lambda z, k, y, x: k)


def partial_sums(place, kernel, labels, *refs):
    parts, totals = refs[:4], refs[4]
    held, cols, rows, sems = refs[5:]
    depth = cols.shape[1]
    zk, at = place[0] // 16, place[0] % 16
    k, y, x = zk % 2, at // 4, at % 4
    starts = []
    for d in range(4):
        for e in range(4):
            outer, inner = y ^ jnp.where(k == 0, e, d), x ^ jnp.where(k == 0, d, e)
            starts.append(pl.multiple_of((outer * 4 + inner) * SLICE, SLICE))
    row_base = pl.multiple_of(zk * rows.shape[1], SLICE)
    col_base = pl.multiple_of(at * depth, SLICE)
    copies = [
        pltpu.make_async_copy(labels.at[:, pl.ds(col_base, cols.shape[1])], cols, sems.at[16]),
        pltpu.make_async_copy(labels.at[:, pl.ds(row_base, rows.shape[1])], rows, sems.at[17]),
    ]
    blocks = []
    for step in range(16):
        blocks.append(
            pltpu.make_async_copy(kernel.at[pl.ds(starts[step], SLICE), :], held.at[step], sems.at[step])
        )
    for copy in copies + blocks:
        copy.start()
    copies[0].wait()
    wide = lax.broadcasted_iota(jnp.int32, (CLUSTERS, depth), 0)
    onehot = jnp.concatenate(
        [(wide == cols[t : t + 1, :]).astype(jnp.float32).astype(jnp.bfloat16) for t in range(ITERS)]
    )
    copies[1].wait()
    narrow = lax.broadcasted_iota(jnp.int32, (CLUSTERS, SLICE), 0)
    sums = [jnp.zeros((CLUSTERS, SLICE), jnp.float32) for _ in range(ITERS)]
    for step, size in WAVES:
        for one in range(step, step + size):
            blocks[one].wait()
        wave = lax.dot_general(
            onehot,
            held[step : step + size].reshape(size * SLICE, depth),
            (((1,), (1,)), ((), ())),
            preferred_element_type=jnp.float32,
        )
        for one in range(step, step + size):
            part = wave[:, (one - step) * SLICE : (one - step + 1) * SLICE]
            parts[one // 4][one % 4] = part
            for t in range(ITERS):
                chosen = narrow == rows[t : t + 1, pl.ds(starts[one], SLICE)]
                sums[t] += jnp.where(chosen, part[t * CLUSTERS : (t + 1) * CLUSTERS], 0.0)
    lines = [jnp.sum(a.T, axis=0, keepdims=True) for a in sums]
    lines.append(jnp.zeros((1, CLUSTERS), jnp.float32))
    both = jnp.concatenate([jnp.concatenate(lines[0:4:2]), jnp.concatenate(lines[1:4:2])], axis=1)
    totals[...] = both


def stage_sum(a, b, c, d, *outs):
    for e in range(4):
        outs[e][...] = (a[e] + b[e]) + (c[e] + d[e])


def tally(labels, after, counts):
    del after
    octet = lax.broadcasted_iota(jnp.int32, (8, SERIES), 0)
    spread = lax.broadcasted_iota(jnp.int32, (8, CLUSTERS), 1) // 8
    keep = spread == lax.broadcasted_iota(jnp.int32, (8, CLUSTERS), 0)
    for t in range(ITERS):
        line = labels[t : t + 1, :]
        high = (octet == line >> 3).astype(jnp.float32).astype(jnp.bfloat16)
        low = (octet == (line & 7)).astype(jnp.float32).astype(jnp.bfloat16)
        square = lax.dot_general(
            high, low, (((1,), (1,)), ((), ())), preferred_element_type=jnp.float32
        )
        row = jnp.sum(jnp.where(keep, jnp.concatenate([square] * 8, axis=1), 0.0), axis=0, keepdims=True)
        counts[t] = jnp.broadcast_to(row, (SLICE, CLUSTERS)).T


def finish(a, b, c, d, counts, shares, distance, objective):
    sums = (a[...] + b[...]) + (c[...] + d[...])
    whole = jnp.sum(shares[...], axis=0)
    whole = (whole[0:2] + whole[2:4]) + (whole[4:6] + whole[6:8])
    for t in range(ITERS):
        row = whole[t // 2 : t // 2 + 1, t % 2 * CLUSTERS : (t % 2 + 1) * CLUSTERS]
        totals = jnp.broadcast_to(row, (SLICE, CLUSTERS)).T
        count = counts[t]
        block = sums[t * CLUSTERS : (t + 1) * CLUSTERS]
        distance[t] = (-2.0 * block) / count + totals / (count * count)
        objective[t] = 1.0 - jnp.sum((totals / count)[:, 0:1]) / SERIES


def near(array):
    return pltpu.with_memory_space_constraint(array, pltpu.VMEM)


def early(part, s):
    return lax.ppermute(part, AXES, first_stage(s))


def vmem():
    return pl.BlockSpec(memory_space=pltpu.VMEM)


def shards(kernel, labels):
    rows_block, cols_block = kernel.shape
    place = lax.axis_index(AXES).reshape(1).astype(jnp.int32)
    block = pltpu.VMEM((4, WIDTH, SLICE), jnp.float32)
    small = pltpu.VMEM((WIDTH, SLICE), jnp.float32)
    *parts, totals = pl.pallas_call(
        partial_sums,
        out_shape=[block] * 4 + [pltpu.VMEM((2, SLICE), jnp.float32)],
        in_specs=[
            pl.BlockSpec(memory_space=pltpu.SMEM),
            pl.BlockSpec(memory_space=pl.ANY),
            pl.BlockSpec(memory_space=pl.ANY),
        ],
        out_specs=[vmem()] * 5,
        scratch_shapes=[
            pltpu.VMEM((16, SLICE, cols_block), jnp.bfloat16),
            pltpu.VMEM((ITERS, cols_block), jnp.int32),
            pltpu.VMEM((ITERS, rows_block), jnp.int32),
            pltpu.SemaphoreType.DMA((18,)),
        ],
    )(place, kernel, labels)
    other = lax.ppermute(totals, "k", [(0, 1), (1, 0)])
    chip = totals + other
    for hop in HOPS:
        other = lax.ppermute(chip, AXES, hop)
        chip = chip + other
    moved = [parts[0]] + [early(parts[s], s) for s in (1, 3, 2)]
    halves = pl.pallas_call(
        stage_sum, out_shape=[small] * 4, in_specs=[vmem()] * 4, out_specs=[vmem()] * 4
    )(*map(near, moved))
    last = [halves[0]]
    for s in (2, 3, 1):
        last.append(lax.ppermute(halves[s], AXES, second_stage(s)))
    counts = pl.pallas_call(
        tally,
        out_shape=pltpu.VMEM((ITERS, CLUSTERS, SLICE), jnp.float32),
        in_specs=[vmem()] * 2,
        out_specs=vmem(),
    )(labels, near(halves[0]))
    shares = lax.all_to_all(
        jnp.broadcast_to(chip[None], (len(GROUPS[0]), 2, SLICE)),
        AXES,
        0,
        0,
        axis_index_groups=GROUPS,
        tiled=True,
    )
    shares = shares.reshape(len(GROUPS[0]) // 4, 8, SLICE)
    distance, objective = pl.pallas_call(
        finish,
        out_shape=[
            jax.ShapeDtypeStruct((ITERS, CLUSTERS, SLICE), jnp.float32),
            jax.ShapeDtypeStruct((ITERS,), jnp.float32),
        ],
        in_specs=[vmem()] * 6,
        out_specs=[vmem(), pl.BlockSpec(memory_space=pltpu.SMEM)],
    )(*map(near, last), near(counts), near(shares))
    return jnp.swapaxes(distance, 1, 2), objective


def solution(mesh):
    finer = Mesh(mesh.devices.reshape(4, 2, 4, 4), AXES)
    return jax.shard_map(
        shards,
        mesh=finer,
        in_specs=(P(("z", "k"), ("y", "x")), P()),
        out_specs=(P(None, AXES, None), P()),
        check_vma=False,
    )
```
